32 devices in a mesh: ta: 4 (over z), sa: 8 (over y, x, core).
Axes of the slice: x: 2, y: 2, z: 4, core: 2. Of those that a mesh axis runs over, the one named last changes fastest.
Arguments:
- frames: float32 [16, 8, 512, 4096], P('ta', 'sa'), may hold values from -6 to 6
- taps: float32 [7], replicated, may hold values from 0.1 to 0.3
Outputs:
- columns: float32 [64, 16, 512, 512], P('sa', 'ta')
The draws below stay inside these ranges and needn't reach their ends.
All inputs are finite; a program needn't handle non-finite values.
Results may differ from the reference program's by a relative error of at most 0.00002.
Values sent between devices are 32-bit elements; how exact they have to be, the bound alone decides.
A program may use at most 256 MiB of HBM per device.

```python
import jax
import jax.numpy as jnp
from jax import lax

NY = 4096
NX = 4096
TS = 512
TIME = 16
READERS = 8
STRIP = 512
TILES = 64
N_SA = 8


def level_of(rng, extent, cuts, low, high):
    gain = 1.0
    for axis_at, blocks in cuts:
        heights = jax.random.uniform(jax.random.fold_in(jax.random.fold_in(rng, 6), axis_at), (blocks,), jnp.float32, low / len(cuts), high / len(cuts))
        gain = gain * jnp.repeat(jnp.exp(heights), extent[axis_at] // blocks).reshape((-1,) + (1,) * (len(extent) - 1 - axis_at))
    return gain


def normal_values(stream_key, shape, deviation, limit, pieces=(), kind=jnp.bfloat16):
    result = deviation * jax.random.normal(stream_key, shape, jnp.float32)
    if pieces:
        result = result * level_of(stream_key, shape, pieces, -0.22, 0.18)
    return jnp.clip(result, -limit, limit).astype(kind)


def setup_inputs(seed: int = 0) -> dict:
    seeds = jax.random.split(jax.random.key(seed), 3)
    return {
        "frames": normal_values(seeds[0], (TIME, READERS, STRIP, NX), 1.0, 6.0, ((0, 4), (1, 8)), jnp.float32),
        "taps": jnp.clip(jax.random.uniform(seeds[1], (7,), jnp.float32, 0.1, 0.3), 0.1, 0.3),
    }


def reference(frames, taps):
    per_tile = TS // N_SA
    tile_rows = NY // TS
    tile_cols = NX // TS

    def one_row(index):
        piece = lax.dynamic_slice_in_dim(frames, index * per_tile, per_tile, 2)
        field = piece.transpose(0, 2, 1, 3).reshape(TIME, TS, NX)
        padded = jnp.pad(field, ((3, 3), (0, 0), (0, 0)))
        total = jnp.zeros_like(field)
        for offset in range(7):
            total = total + taps[offset] * padded[offset:offset + TIME]
        return total.reshape(TIME, TS, tile_cols, TS).transpose(2, 0, 1, 3)

    stacked = lax.map(one_row, jnp.arange(tile_rows, dtype=jnp.int32))
    return stacked.reshape(TILES, TIME, TS, TS)
```

```python
import functools

import jax
import jax.numpy as jnp
from jax import lax
from jax.experimental import pallas as pl
from jax.experimental.pallas import tpu as pltpu
from jax.sharding import PartitionSpec as P

TS = 512
REACH = 3
SUBLANES = 8
LATE = 2
LATE_UNITS = (2, 1)


def partner(me, m, n, sign):
    if n & (n - 1):
        return (me + sign * m + n) % n
    other, bit = me, 1
    while bit < n:
        if m & bit:
            other = other + bit * (1 - 2 * ((me // bit) % 2))
        bit *= 2
    return other


def late_pieces(late, rows):
    pieces = [(tile, 0, rows) for tile in range(late)]
    units = rows // SUBLANES
    if late and units > sum(LATE_UNITS):
        sizes = (units - sum(LATE_UNITS),) + LATE_UNITS
        pieces[-1:] = [(late - 1, sum(sizes[:i]) * SUBLANES, size * SUBLANES) for i, size in enumerate(sizes)]
    return pieces


def exchange_kernel(groups, n, rows, width, sent, pieces, frames, *refs):
    late = sent < width
    stage, low, high = refs[:3]
    heads, tails = refs[3:3 + len(pieces)], refs[3 + len(pieces):3 + 2 * len(pieces)]
    own, own_sem, a_send, a_recv, up_send, up_recv, down_send, down_recv = refs[3 + 2 * len(pieces):][:8]
    if late:
        late_cells, late_load, late_store = refs[-3:]
    steps = frames.shape[0]
    group, me = lax.axis_index("ta"), lax.axis_index("sa")
    across = frames.shape[3] // width
    order = sorted(range(1, n), key=lambda m: (bin(m >> 1).count("1"), m & 1, m))
    parts = [(0, sent), (sent, width - sent)] if late else [(0, width)]
    has_prev, has_next = group > 0, group < groups - 1
    leads = me % 2 == 0
    follows = jnp.logical_not(leads)

    def cells_for(owner, first, count):
        row = pl.ds(pl.multiple_of((owner // across) * rows, 8), rows)
        col = pl.ds(pl.multiple_of((owner % across) * width + first, TS), count)
        return frames.at[:, 0, row, col]

    barrier = pltpu.get_barrier_semaphore()
    for m in order:
        pl.semaphore_signal(barrier, inc=1, device_id={"sa": partner(me, m, n, 1)})

    @pl.when(has_prev)
    def _():
        pl.semaphore_signal(barrier, inc=1, device_id={"ta": group - 1})

    @pl.when(has_next)
    def _():
        pl.semaphore_signal(barrier, inc=1, device_id={"ta": group + 1})

    def block_copy(m, part):
        first, count = parts[part]
        return pltpu.make_async_remote_copy(
            src_ref=cells_for(partner(me, m, n, 1), first, count), dst_ref=stage.at[me, :, :, pl.ds(first, count)],
            send_sem=a_send.at[part, m], recv_sem=a_recv.at[part, m], device_id={"sa": partner(me, m, n, 1)})

    def edge_copy(m, which):
        source = partner(me, m, n, -1)
        cells = cells_for(me, 0, sent) if m == 0 else stage.at[source, :, :, pl.ds(0, sent)]
        if which == "up":
            return pltpu.make_async_remote_copy(
                src_ref=cells.at[pl.ds(steps - REACH, REACH)], dst_ref=low.at[source],
                send_sem=up_send.at[m], recv_sem=up_recv.at[m], device_id={"ta": group + 1})
        return pltpu.make_async_remote_copy(
            src_ref=cells.at[pl.ds(0, REACH)], dst_ref=high.at[source],
            send_sem=down_send.at[m], recv_sem=down_recv.at[m], device_id={"ta": group - 1})

    def send_edges(m):
        @pl.when(has_next)
        def _():
            edge_copy(m, "up").start()

        @pl.when(has_prev)
        def _():
            edge_copy(m, "down").start()

    def late_copies(m):
        source = partner(me, m, n, -1)
        copies = []
        for p, (tile, first, count) in enumerate(pieces):
            row, col = pl.ds(first, count), pl.ds(tile * TS, TS)
            copies += [
                pltpu.make_async_copy(
                    late_cells.at[m, pl.ds(steps - REACH, REACH), row, col], tails[p].at[source], late_store.at[0, p, m]),
                pltpu.make_async_copy(
                    late_cells.at[m, pl.ds(0, REACH), row, col], heads[p].at[source], late_store.at[1, p, m]),
            ]
        return copies

    def take_late(m):
        if m == 0:
            cells = cells_for(me, *parts[-1])
        else:
            cells = stage.at[partner(me, m, n, -1), :, :, pl.ds(*parts[-1])]
        taken = pltpu.make_async_copy(cells, late_cells.at[m], late_load.at[m])
        taken.start()
        taken.wait()
        for put in late_copies(m):
            put.start()

    load = pltpu.make_async_copy(cells_for(me, 0, width), own, own_sem.at[0])
    load.start()

    neighbours = jnp.where(has_prev, 1, 0) + jnp.where(has_next, 1, 0)
    pl.semaphore_wait(barrier, n - 1 + neighbours)

    @pl.when(leads)
    def _():
        send_edges(0)

    for m in order[1:]:
        block_copy(m, 0).start()

    @pl.when(follows)
    def _():
        block_copy(order[0], 0).start()

    if late:
        for m in order:
            block_copy(m, 1).start()
    load.wait()
    store = pltpu.make_async_copy(own, stage.at[me], own_sem.at[1])
    store.start()
    for m in order:
        block_copy(m, 0).wait_recv()
        if m == order[0]:
            @pl.when(leads)
            def _():
                block_copy(m, 0).start()

            @pl.when(follows)
            def _():
                send_edges(0)
        send_edges(m)
    if late:
        take_late(0)
        for m in order:
            block_copy(m, 1).wait_recv()
            take_late(m)
    store.wait()
    if late:
        for m in [0] + order:
            for put in late_copies(m):
                put.wait()
    for part in range(len(parts)):
        for m in order:
            block_copy(m, part).wait_send()
    for m in [0] + order:
        @pl.when(has_next)
        def _():
            edge_copy(m, "up").wait_send()
            edge_copy(m, "down").wait_recv()

        @pl.when(has_prev)
        def _():
            edge_copy(m, "down").wait_send()
            edge_copy(m, "up").wait_recv()


def exchanged(frames, groups, n, rows, width, sent, pieces):
    steps = frames.shape[0]
    any_space = pl.BlockSpec(memory_space=pl.ANY)
    edge = jax.ShapeDtypeStruct((n, REACH, rows, sent), jnp.float32)
    dma, block_dma = pltpu.SemaphoreType.DMA((n,)), pltpu.SemaphoreType.DMA((2, n))
    shapes = [jax.ShapeDtypeStruct((n, steps, rows, width), jnp.float32), edge, edge]
    scratch = [pltpu.VMEM((steps, rows, width), jnp.float32), pltpu.SemaphoreType.DMA((2,)), block_dma, block_dma] + [dma] * 4
    if pieces:
        shapes += [jax.ShapeDtypeStruct((n, REACH, count, TS), jnp.float32) for _, _, count in pieces] * 2
        scratch += [
            pltpu.VMEM((n, steps, rows, width - sent), jnp.float32), dma, pltpu.SemaphoreType.DMA((2, len(pieces), n))]
    return pl.pallas_call(
        functools.partial(exchange_kernel, groups, n, rows, width, sent, pieces),
        out_shape=shapes,
        in_specs=[any_space],
        out_specs=[any_space] * len(shapes),
        scratch_shapes=scratch,
        compiler_params=pltpu.CompilerParams(collective_id=0, has_side_effects=True),
        name="exchange",
    )(frames)


def smooth_kernel(groups, taps, stage, low, high, *rest):
    out, woven = rest[-2:]
    n, steps, rows, cols = stage.shape
    group = lax.axis_index("ta")
    first, last = group == 0, group == groups - 1
    weights = [taps[j] for j in range(2 * REACH + 1)]

    for c in range(0, cols, 128):
        lanes = pl.ds(c, 128)

        def one_source(s, carry):
            for r in range(0, rows, 8):
                at = (pl.ds(r, 8), lanes)
                lo = [jnp.where(first, 0.0, low[(s, j) + at]) for j in range(REACH)]
                hi = [jnp.where(last, 0.0, high[(s, j) + at]) for j in range(REACH)]
                cells = lo + [stage[(s, t) + at] for t in range(steps)] + hi
                for t in range(steps):
                    total = weights[0] * cells[t]
                    for j in range(1, 2 * REACH + 1):
                        total = total + weights[j] * cells[t + j]
                    woven[t, pl.ds(r * n + s, 8, stride=n), :] = total
            return carry

        lax.fori_loop(0, n, one_source, 0)
        for t in range(steps):
            out[t, :, lanes] = woven[t]


def smoothed(taps, stage, low, high, groups, tiles, band, height, col_tiles, owned, into=None):
    n, steps = stage.shape[:2]
    (start, count), (first, span) = tiles, band
    splits, above = (TS // n) // height, first // height

    def cells_at(k, h):
        return 0, 0, ((k + start) // col_tiles) * splits + above + h, (k + start) % col_tiles

    def edges_at(k, h):
        return cells_at(k, h) if into is None else (0, 0, h, 0)

    specs = [
        pl.BlockSpec(memory_space=pltpu.SMEM),
        pl.BlockSpec((n, steps, height, TS), cells_at),
        pl.BlockSpec((n, REACH, height, TS), edges_at),
        pl.BlockSpec((n, REACH, height, TS), edges_at),
    ]
    operands = [taps, stage, low, high]
    if into is not None:
        specs.append(pl.BlockSpec(memory_space=pl.ANY))
        operands.append(into)
    moved = count * steps * span * n * TS * 4
    return pl.pallas_call(
        functools.partial(smooth_kernel, groups),
        grid=(count, span // height),
        out_shape=jax.ShapeDtypeStruct((owned, steps, TS, TS), jnp.float32),
        in_specs=specs,
        out_specs=pl.BlockSpec((None, steps, height * n, TS), lambda k, h: (k + start, 0, above + h, 0)),
        scratch_shapes=[pltpu.VMEM((steps, height * n, 128), jnp.float32)],
        input_output_aliases={} if into is None else {4: 0},
        compiler_params=pltpu.CompilerParams(vmem_limit_bytes=60 * 1024 * 1024),
        cost_estimate=pl.CostEstimate(flops=moved * 4, bytes_accessed=moved * 7 // 2, transcendentals=0),
        name="smooth",
    )(*operands)


def on_device(frames, taps):
    groups, n = lax.axis_size("ta"), lax.axis_size("sa")
    tile_rows, tile_cols = frames.shape[2] * n // TS, frames.shape[3] // TS
    owned = tile_rows * tile_cols // n
    col_tiles = min(owned, tile_cols)
    width = col_tiles * TS
    per_tile = TS // n
    rows = max(1, owned // tile_cols) * per_tile
    late = LATE if owned == col_tiles and col_tiles > LATE else 0
    pieces = late_pieces(late, per_tile)
    stage, low, high, *edges = exchanged(frames, groups, n, rows, width, width - late * TS, pieces)
    heads, tails = edges[:len(pieces)], edges[len(pieces):]
    ups, downs = [(i, i + 1) for i in range(groups - 1)], [(i + 1, i) for i in range(groups - 1)]
    late_edges = [(lax.ppermute(tail, "ta", ups), lax.ppermute(head, "ta", downs)) for head, tail in zip(heads, tails)]
    height = min(per_tile, max(SUBLANES, 256 // n))
    out = smoothed(taps, stage, low, high, groups, (0, owned - late), (0, per_tile), height, col_tiles, owned)
    for (tile, first, count), (late_low, late_high) in zip(pieces, late_edges):
        step = height if count == per_tile else min(SUBLANES, count)
        out = smoothed(
            taps, stage, late_low, late_high, groups, (owned - late + tile, 1), (first, count), step, col_tiles, owned, out)
    return out


def solution(mesh):
    placed = (P("ta", "sa", None, None), P())
    return jax.shard_map(
        on_device, mesh=mesh, in_specs=placed, out_specs=P("sa", "ta", None, None), check_vma=False
    )
```

```python
import functools

import jax
import jax.numpy as jnp
from jax import lax
from jax.experimental import pallas as pl
from jax.experimental.pallas import tpu as pltpu
from jax.sharding import PartitionSpec as P

TS = 512
REACH = 3
SUBLANES = 8
LATE = 2
LATE_UNITS = (2, 1)


def partner(me, m, n, sign):
    if n & (n - 1):
        return (me + sign * m + n) % n
    other, bit = me, 1
    while bit < n:
        if m & bit:
            other = other + bit * (1 - 2 * ((me // bit) % 2))
        bit *= 2
    return other


def greeted_first(order, n):
    if n & (n - 1):
        return order, {}
    near = [m for m in order if m & (m - 1) == 0]
    vouchers = {}
    for m in order:
        if m not in near:
            vouchers.setdefault(next(v for v in order if v & m == v and bin(m ^ v).count("1") == 1), []).append(m)
    return near, vouchers


def late_pieces(late, rows):
    pieces = [(tile, 0, rows) for tile in range(late)]
    units = rows // SUBLANES
    if late and units > sum(LATE_UNITS):
        sizes = (units - sum(LATE_UNITS),) + LATE_UNITS
        pieces[-1:] = [(late - 1, sum(sizes[:i]) * SUBLANES, size * SUBLANES) for i, size in enumerate(sizes)]
    return pieces


def exchange_kernel(groups, n, rows, width, sent, pieces, frames, *refs):
    late = sent < width
    stage, low, high = refs[:3]
    held, heads, tails = (refs[3 + i * len(pieces):3 + (i + 1) * len(pieces)] for i in range(3))
    own, own_sem, a_send, a_recv, up_send, up_recv, down_send, down_recv = refs[3 + 3 * len(pieces):][:8]
    if late:
        late_cells, late_load, late_store = refs[-3:]
    steps = frames.shape[0]
    group, me = lax.axis_index("ta"), lax.axis_index("sa")
    across = frames.shape[3] // width
    order = sorted(range(1, n), key=lambda m: (bin(m >> 1).count("1"), m & 1, m))
    parts = [(0, sent), (sent, width - sent)] if late else [(0, width)]
    has_prev, has_next = group > 0, group < groups - 1
    leads = me % 2 == 0
    follows = jnp.logical_not(leads)

    def cells_for(owner, first, count):
        row = pl.ds(pl.multiple_of((owner // across) * rows, 8), rows)
        col = pl.ds(pl.multiple_of((owner % across) * width + first, TS), count)
        return frames.at[:, 0, row, col]

    near, vouchers = greeted_first(order, n)
    barrier = pltpu.get_barrier_semaphore()

    @pl.when(has_prev)
    def _():
        pl.semaphore_signal(barrier, inc=1, device_id={"ta": group - 1})

    @pl.when(has_next)
    def _():
        pl.semaphore_signal(barrier, inc=1, device_id={"ta": group + 1})

    for m in near:
        pl.semaphore_signal(barrier, inc=1, device_id={"sa": partner(me, m, n, 1)})

    load = pltpu.make_async_copy(cells_for(me, *parts[0]), own, own_sem.at[0])
    load.start()

    def block_copy(m, part):
        return pltpu.make_async_remote_copy(
            src_ref=cells_for(partner(me, m, n, 1), *parts[part]), dst_ref=late_cells.at[m] if part else stage.at[me],
            send_sem=a_send.at[part, m], recv_sem=a_recv.at[part, m], device_id={"sa": partner(me, m, n, 1)})

    def edge_copy(m, which):
        source = partner(me, m, n, -1)
        cells = own if m == 0 else stage.at[source]
        if which == "up":
            return pltpu.make_async_remote_copy(
                src_ref=cells.at[pl.ds(steps - REACH, REACH)], dst_ref=low.at[source],
                send_sem=up_send.at[m], recv_sem=up_recv.at[m], device_id={"ta": group + 1})
        return pltpu.make_async_remote_copy(
            src_ref=cells.at[pl.ds(0, REACH)], dst_ref=high.at[source],
            send_sem=down_send.at[m], recv_sem=down_recv.at[m], device_id={"ta": group - 1})

    def send_edges(m):
        @pl.when(has_next)
        def _():
            edge_copy(m, "up").start()

        @pl.when(has_prev)
        def _():
            edge_copy(m, "down").start()

    def late_copies(m):
        source = partner(me, m, n, -1)
        copies = []
        for p, (tile, first, count) in enumerate(pieces):
            row, col = pl.ds(first, count), pl.ds(tile * TS, TS)
            moves = (
                (pl.ds(0, steps), held[p]), (pl.ds(steps - REACH, REACH), tails[p]), (pl.ds(0, REACH), heads[p]))
            copies += [
                pltpu.make_async_copy(late_cells.at[m, step, row, col], target.at[source], late_store.at[i, p, m])
                for i, (step, target) in enumerate(moves)]
        return copies

    def put_late(m):
        for put in late_copies(m):
            put.start()

    neighbours = jnp.where(has_prev, 1, 0) + jnp.where(has_next, 1, 0)
    pl.semaphore_wait(barrier, len(near) + neighbours)
    load.wait()

    @pl.when(leads)
    def _():
        send_edges(0)

    for m in near[1:]:
        block_copy(m, 0).start()

    @pl.when(follows)
    def _():
        block_copy(order[0], 0).start()

    store = pltpu.make_async_copy(own, stage.at[me], own_sem.at[1])
    store.start()
    if late:
        late_own = pltpu.make_async_copy(cells_for(me, *parts[1]), late_cells.at[0], late_load.at[0])
        late_own.start()
    left = n - 1 - len(near)

    def start_late():
        if late:
            for m in order:
                block_copy(m, 1).start()

    if not left:
        start_late()
    for m in order:
        block_copy(m, 0).wait_recv()
        if m == order[0]:
            @pl.when(leads)
            def _():
                block_copy(m, 0).start()

            @pl.when(follows)
            def _():
                send_edges(0)
        send_edges(m)
        for other in vouchers.get(m, []):
            block_copy(other, 0).start()
            left -= 1
            if not left:
                start_late()
    if late:
        late_own.wait()
        put_late(0)
        for m in order:
            block_copy(m, 1).wait_recv()
            put_late(m)
    store.wait()
    if late:
        for m in [0] + order:
            for put in late_copies(m):
                put.wait()
    for part in range(len(parts)):
        for m in order:
            block_copy(m, part).wait_send()
    for m in [0] + order:
        @pl.when(has_next)
        def _():
            edge_copy(m, "up").wait_send()
            edge_copy(m, "down").wait_recv()

        @pl.when(has_prev)
        def _():
            edge_copy(m, "down").wait_send()
            edge_copy(m, "up").wait_recv()


def exchanged(frames, groups, n, rows, width, sent, pieces):
    steps = frames.shape[0]
    any_space = pl.BlockSpec(memory_space=pl.ANY)
    edge = jax.ShapeDtypeStruct((n, REACH, rows, sent), jnp.float32)
    dma, block_dma = pltpu.SemaphoreType.DMA((n,)), pltpu.SemaphoreType.DMA((2, n))
    shapes = [jax.ShapeDtypeStruct((n, steps, rows, sent), jnp.float32), edge, edge]
    scratch = [pltpu.VMEM((steps, rows, sent), jnp.float32), pltpu.SemaphoreType.DMA((2,)), block_dma, block_dma] + [dma] * 4
    if pieces:
        shapes += [
            jax.ShapeDtypeStruct((n, depth, count, TS), jnp.float32)
            for depth in (steps, REACH, REACH) for _, _, count in pieces]
        scratch += [
            pltpu.VMEM((n, steps, rows, width - sent), jnp.float32), pltpu.SemaphoreType.DMA((1,)),
            pltpu.SemaphoreType.DMA((3, len(pieces), n))]
    return pl.pallas_call(
        functools.partial(exchange_kernel, groups, n, rows, width, sent, pieces),
        out_shape=shapes,
        in_specs=[any_space],
        out_specs=[any_space] * len(shapes),
        scratch_shapes=scratch,
        compiler_params=pltpu.CompilerParams(collective_id=0, has_side_effects=True),
        name="exchange",
    )(frames)


def smooth_kernel(groups, taps, stage, low, high, *rest):
    out, woven = rest[-2:]
    n, steps, rows, cols = stage.shape
    group = lax.axis_index("ta")
    first, last = group == 0, group == groups - 1
    weights = [taps[j] for j in range(2 * REACH + 1)]

    for c in range(0, cols, 128):
        lanes = pl.ds(c, 128)

        def one_source(s, carry):
            for r in range(0, rows, 8):
                at = (pl.ds(r, 8), lanes)
                lo = [jnp.where(first, 0.0, low[(s, j) + at]) for j in range(REACH)]
                hi = [jnp.where(last, 0.0, high[(s, j) + at]) for j in range(REACH)]
                cells = lo + [stage[(s, t) + at] for t in range(steps)] + hi
                for t in range(steps):
                    total = weights[0] * cells[t]
                    for j in range(1, 2 * REACH + 1):
                        total = total + weights[j] * cells[t + j]
                    woven[t, pl.ds(r * n + s, 8, stride=n), :] = total
            return carry

        if rows == SUBLANES and n <= SUBLANES:
            for s in range(n):
                one_source(s, 0)
        else:
            lax.fori_loop(0, n, one_source, 0)
        for t in range(steps):
            out[t, :, lanes] = woven[t]


def smoothed(taps, stage, low, high, groups, tiles, band, height, col_tiles, owned, into=None):
    n, steps = stage.shape[:2]
    (start, count), (first, span) = tiles, band
    splits, above = (TS // n) // height, first // height

    def cells_at(k, h):
        if into is not None:
            return 0, 0, h, 0
        return 0, 0, ((k + start) // col_tiles) * splits + h, (k + start) % col_tiles

    specs = [
        pl.BlockSpec(memory_space=pltpu.SMEM),
        pl.BlockSpec((n, steps, height, TS), cells_at),
        pl.BlockSpec((n, REACH, height, TS), cells_at),
        pl.BlockSpec((n, REACH, height, TS), cells_at),
    ]
    operands = [taps, stage, low, high]
    if into is not None:
        specs.append(pl.BlockSpec(memory_space=pl.ANY))
        operands.append(into)
    moved = count * steps * span * n * TS * 4
    return pl.pallas_call(
        functools.partial(smooth_kernel, groups),
        grid=(count, span // height),
        out_shape=jax.ShapeDtypeStruct((owned, steps, TS, TS), jnp.float32),
        in_specs=specs,
        out_specs=pl.BlockSpec((None, steps, height * n, TS), lambda k, h: (k + start, 0, above + h, 0)),
        scratch_shapes=[pltpu.VMEM((steps, height * n, 128), jnp.float32)],
        input_output_aliases={} if into is None else {4: 0},
        compiler_params=pltpu.CompilerParams(vmem_limit_bytes=(40 if height > SUBLANES else 8) * 1024 * 1024),
        cost_estimate=pl.CostEstimate(flops=moved * 4, bytes_accessed=moved * 7 // 2, transcendentals=0),
        name="smooth",
    )(*operands)


def on_device(frames, taps):
    groups, n = lax.axis_size("ta"), lax.axis_size("sa")
    tile_rows, tile_cols = frames.shape[2] * n // TS, frames.shape[3] // TS
    owned = tile_rows * tile_cols // n
    col_tiles = min(owned, tile_cols)
    width = col_tiles * TS
    per_tile = TS // n
    rows = max(1, owned // tile_cols) * per_tile
    late = LATE if owned == col_tiles and col_tiles > LATE else 0
    pieces = late_pieces(late, per_tile)
    stage, low, high, *edges = exchanged(frames, groups, n, rows, width, width - late * TS, pieces)
    held, heads, tails = (edges[i * len(pieces):(i + 1) * len(pieces)] for i in range(3))
    ups, downs = [(i, i + 1) for i in range(groups - 1)], [(i + 1, i) for i in range(groups - 1)]
    late_edges = [(lax.ppermute(tail, "ta", ups), lax.ppermute(head, "ta", downs)) for head, tail in zip(heads, tails)]
    height = min(per_tile, max(SUBLANES, 256 // n))
    out = smoothed(taps, stage, low, high, groups, (0, owned - late), (0, per_tile), height, col_tiles, owned)
    for (tile, first, count), cells, (late_low, late_high) in zip(pieces, held, late_edges):
        step = height if count == per_tile else min(SUBLANES, count)
        out = smoothed(
            taps, cells, late_low, late_high, groups, (owned - late + tile, 1), (first, count), step, col_tiles, owned, out)
    return out


def solution(mesh):
    placed = (P("ta", "sa", None, None), P())
    return jax.shard_map(
        on_device, mesh=mesh, in_specs=placed, out_specs=P("sa", "ta", None, None), check_vma=False
    )
```

```python
import functools

import jax
import jax.numpy as jnp
from jax import lax
from jax.experimental import pallas as pl
from jax.experimental.pallas import tpu as pltpu
from jax.sharding import PartitionSpec as P

TS = 512
REACH = 3
SUBLANES = 8
LATE = 2
LATE_UNITS = (2, 1)
LATE_HALVES = 2


def partner(me, m, n, sign):
    if n & (n - 1):
        return (me + sign * m + n) % n
    other, bit = me, 1
    while bit < n:
        if m & bit:
            other = other + bit * (1 - 2 * ((me // bit) % 2))
        bit *= 2
    return other


def greeted_first(order, n):
    if n & (n - 1):
        return order, {}
    near = [m for m in order if m & (m - 1) == 0]
    vouchers = {}
    for m in order:
        if m not in near:
            vouchers.setdefault(next(v for v in order if v & m == v and bin(m ^ v).count("1") == 1), []).append(m)
    return near, vouchers


def late_pieces(late, rows):
    pieces = [(tile, 0, rows, 0, TS) for tile in range(late)]
    units = rows // SUBLANES
    if late and units > sum(LATE_UNITS):
        sizes = (units - sum(LATE_UNITS),) + LATE_UNITS
        pieces[-1:] = [(late - 1, sum(sizes[:i]) * SUBLANES, size * SUBLANES, 0, TS) for i, size in enumerate(sizes)]
        tile, first, count = pieces.pop()[:3]
        pieces += [(tile, first, count, col, TS // LATE_HALVES) for col in range(0, TS, TS // LATE_HALVES)]
    return pieces


def exchange_kernel(groups, n, rows, width, sent, pieces, frames, *refs):
    late = sent < width
    stage, low, high = refs[:3]
    held, heads, tails = (refs[3 + i * len(pieces):3 + (i + 1) * len(pieces)] for i in range(3))
    (own, own_sem, a_send, a_recv, up_send, up_recv, down_send, down_recv,
     next_in, beside_in, near_in) = refs[3 + 3 * len(pieces):][:11]
    if late:
        late_cells, late_load, late_store = refs[-3:]
    steps = frames.shape[0]
    group, me = lax.axis_index("ta"), lax.axis_index("sa")
    across = frames.shape[3] // width
    order = sorted(range(1, n), key=lambda m: (bin(m >> 1).count("1"), m & 1, m))
    parts = [(0, sent), (sent, width - sent)] if late else [(0, width)]
    has_prev, has_next = group > 0, group < groups - 1
    leads = me % 2 == 0
    follows = jnp.logical_not(leads)

    def cells_for(owner, first, count):
        row = pl.ds(pl.multiple_of((owner // across) * rows, 8), rows)
        col = pl.ds(pl.multiple_of((owner % across) * width + first, TS), count)
        return frames.at[:, 0, row, col]

    def await_own():
        @pl.when(has_next)
        def _():
            edge_copy(awaited, "up").wait_send()

        @pl.when(has_prev)
        def _():
            edge_copy(awaited, "down").wait_send()

    opening = min(SUBLANES, rows)
    spans = {0: (0, opening), n: (opening, rows - opening)}
    edges = [m for m in [0, n] + order if spans.get(m, (0, rows))[1]]
    own_edges = [m for m in edges if m in spans]
    awaited = own_edges[-1]
    mine = cells_for(me, *parts[0])
    loads = [
        pltpu.make_async_copy(mine.at[:, pl.ds(*spans[m])], own.at[:, pl.ds(*spans[m])], own_sem.at[1 + i])
        for i, m in enumerate(own_edges)]

    for load in loads:
        load.start()

    near, vouchers = greeted_first(order, n)
    barrier = pltpu.get_barrier_semaphore()

    @pl.when(has_next)
    def _():
        pl.semaphore_signal(barrier, inc=1, device_id={"ta": group + 1})

    @pl.when(jnp.logical_not(has_prev))
    def _():
        for m in near:
            pl.semaphore_signal(barrier, inc=1, device_id={"sa": partner(me, m, n, 1)})


    def block_copy(m, part):
        return pltpu.make_async_remote_copy(
            src_ref=cells_for(partner(me, m, n, 1), *parts[part]), dst_ref=late_cells.at[m] if part else stage.at[me],
            send_sem=a_send.at[part, m], recv_sem=a_recv.at[part, m], device_id={"sa": partner(me, m, n, 1)})

    def edge_copy(m, which):
        source, row = partner(me, m % n, n, -1), pl.ds(*spans.get(m, (0, rows)))
        cells = own if m in spans else stage.at[source]
        if which == "up":
            return pltpu.make_async_remote_copy(
                src_ref=cells.at[pl.ds(steps - REACH, REACH), row], dst_ref=low.at[source, :, row],
                send_sem=up_send.at[m], recv_sem=up_recv.at[m], device_id={"ta": group + 1})
        return pltpu.make_async_remote_copy(
            src_ref=cells.at[pl.ds(0, REACH), row], dst_ref=high.at[source, :, row],
            send_sem=down_send.at[m], recv_sem=down_recv.at[m], device_id={"ta": group - 1})

    def send_edges(m, which=("up", "down")):
        if m not in edges:
            return
        for way in which:
            @pl.when(has_next if way == "up" else has_prev)
            def _():
                edge_copy(m, way).start()

    def late_copies(m):
        source = partner(me, m, n, -1)
        copies = []
        for p, (tile, first, count, left, wide) in enumerate(pieces):
            row, col = pl.ds(first, count), pl.ds(tile * TS + left, wide)
            moves = (
                (pl.ds(0, steps), held[p]), (pl.ds(steps - REACH, REACH), tails[p]), (pl.ds(0, REACH), heads[p]))
            copies += [
                pltpu.make_async_copy(late_cells.at[m, step, row, col], target.at[source], late_store.at[i, p, m])
                for i, (step, target) in enumerate(moves)]
        return copies

    def put_late(m):
        for put in late_copies(m):
            put.start()

    pl.semaphore_wait(barrier, jnp.where(has_prev, 1, len(near)))

    @pl.when(has_prev)
    def _():
        pl.semaphore_signal(next_in, inc=1, device_id={"ta": group - 1})

    for load, m in zip(loads, own_edges):
        load.wait()

        @pl.when(leads)
        def _():
            send_edges(m, ["down"])

    @pl.when(has_next)
    def _():
        pl.semaphore_wait(next_in, 1)

    @pl.when(leads)
    def _():
        send_edges(0, ["up"])
        send_edges(n, ["up"])

    @pl.when(has_prev)
    def _():
        pl.semaphore_wait(near_in, 1)

    for m in near[1:]:
        block_copy(m, 0).start()

    @pl.when(follows)
    def _():
        block_copy(order[0], 0).start()

    @pl.when(has_next)
    def _():
        for m in near:
            pl.semaphore_signal(beside_in, inc=1, device_id={"sa": partner(me, m, n, 1)})
        pl.semaphore_wait(beside_in, len(near))
        pl.semaphore_signal(near_in, inc=1, device_id={"ta": group + 1})

    store = pltpu.make_async_copy(own, stage.at[me], own_sem.at[0])
    store.start()
    if late:
        late_own = pltpu.make_async_copy(cells_for(me, *parts[1]), late_cells.at[0], late_load.at[0])
        late_own.start()
    for m in order:
        block_copy(m, 0).wait_recv()
        if m == order[0]:
            @pl.when(follows)
            def _():
                send_edges(0)
                send_edges(n)
        send_edges(m)
        if m == order[0]:
            @pl.when(leads)
            def _():
                await_own()
                block_copy(m, 0).start()

        for other in vouchers.get(m, []):
            block_copy(other, 0).start()
    if late:
        for m in order:
            block_copy(m, 1).start()
        late_own.wait()
        put_late(0)
        for m in order:
            block_copy(m, 1).wait_recv()
            put_late(m)
    store.wait()
    if late:
        for m in [0] + order:
            for put in late_copies(m):
                put.wait()
    for part in range(len(parts)):
        for m in order:
            block_copy(m, part).wait_send()
    @pl.when(follows)
    def _():
        await_own()

    for m in edges:
        @pl.when(has_next)
        def _():
            if m != awaited:
                edge_copy(m, "up").wait_send()
            edge_copy(m, "down").wait_recv()

        @pl.when(has_prev)
        def _():
            if m != awaited:
                edge_copy(m, "down").wait_send()
            edge_copy(m, "up").wait_recv()


def exchanged(frames, groups, n, rows, width, sent, pieces):
    steps = frames.shape[0]
    any_space = pl.BlockSpec(memory_space=pl.ANY)
    edge = jax.ShapeDtypeStruct((n, REACH, rows, sent), jnp.float32)
    dma, block_dma = pltpu.SemaphoreType.DMA((n + 1,)), pltpu.SemaphoreType.DMA((2, n))
    shapes = [jax.ShapeDtypeStruct((n, steps, rows, sent), jnp.float32), edge, edge]
    scratch = [pltpu.VMEM((steps, rows, sent), jnp.float32), pltpu.SemaphoreType.DMA((3,)), block_dma, block_dma] + [dma] * 4
    scratch += [pltpu.SemaphoreType.REGULAR] * 3
    if pieces:
        shapes += [
            jax.ShapeDtypeStruct((n, depth, count, wide), jnp.float32)
            for depth in (steps, REACH, REACH) for _, _, count, _, wide in pieces]
        scratch += [
            pltpu.VMEM((n, steps, rows, width - sent), jnp.float32), pltpu.SemaphoreType.DMA((1,)),
            pltpu.SemaphoreType.DMA((3, len(pieces), n))]
    return pl.pallas_call(
        functools.partial(exchange_kernel, groups, n, rows, width, sent, pieces),
        out_shape=shapes,
        in_specs=[any_space],
        out_specs=[any_space] * len(shapes),
        scratch_shapes=scratch,
        compiler_params=pltpu.CompilerParams(collective_id=0, has_side_effects=True),
        name="exchange",
    )(frames)


def smooth_kernel(groups, taps, stage, low, high, *rest):
    out, woven = rest[-2:]
    n, steps, rows, cols = stage.shape
    group = lax.axis_index("ta")
    first, last = group == 0, group == groups - 1
    weights = [taps[j] for j in range(2 * REACH + 1)]

    for c in range(0, cols, 128):
        lanes = pl.ds(c, 128)

        def one_source(s, carry):
            for r in range(0, rows, 8):
                at = (pl.ds(r, 8), lanes)
                lo = [jnp.where(first, 0.0, low[(s, j) + at]) for j in range(REACH)]
                hi = [jnp.where(last, 0.0, high[(s, j) + at]) for j in range(REACH)]
                cells = lo + [stage[(s, t) + at] for t in range(steps)] + hi
                for t in range(steps):
                    total = weights[0] * cells[t]
                    for j in range(1, 2 * REACH + 1):
                        total = total + weights[j] * cells[t + j]
                    woven[t, pl.ds(r * n + s, 8, stride=n), :] = total
            return carry

        if rows == SUBLANES and n <= SUBLANES:
            for s in range(n):
                one_source(s, 0)
        else:
            lax.fori_loop(0, n, one_source, 0)
        for t in range(steps):
            out[t, :, lanes] = woven[t]


def smoothed(taps, stage, low, high, groups, tiles, band, cols, height, col_tiles, owned, into=None):
    n, steps = stage.shape[:2]
    (start, count), (first, span), (left, wide) = tiles, band, cols
    splits, above = (TS // n) // height, first // height

    def cells_at(k, h):
        if into is not None:
            return 0, 0, h, 0
        return 0, 0, ((k + start) // col_tiles) * splits + h, (k + start) % col_tiles

    specs = [
        pl.BlockSpec(memory_space=pltpu.SMEM),
        pl.BlockSpec((n, steps, height, wide), cells_at),
        pl.BlockSpec((n, REACH, height, wide), cells_at),
        pl.BlockSpec((n, REACH, height, wide), cells_at),
    ]
    operands = [taps, stage, low, high]
    if into is not None:
        specs.append(pl.BlockSpec(memory_space=pl.ANY))
        operands.append(into)
    moved = count * steps * span * n * wide * 4
    return pl.pallas_call(
        functools.partial(smooth_kernel, groups),
        grid=(count, span // height),
        out_shape=jax.ShapeDtypeStruct((owned, steps, TS, TS), jnp.float32),
        in_specs=specs,
        out_specs=pl.BlockSpec((None, steps, height * n, wide), lambda k, h: (k + start, 0, above + h, left // wide)),
        scratch_shapes=[pltpu.VMEM((steps, height * n, 128), jnp.float32)],
        input_output_aliases={} if into is None else {4: 0},
        compiler_params=pltpu.CompilerParams(vmem_limit_bytes=(40 if height > SUBLANES else 8) * 1024 * 1024),
        cost_estimate=pl.CostEstimate(flops=moved * 4, bytes_accessed=moved * 7 // 2, transcendentals=0),
        name="smooth",
    )(*operands)


def on_device(frames, taps):
    groups, n = lax.axis_size("ta"), lax.axis_size("sa")
    tile_rows, tile_cols = frames.shape[2] * n // TS, frames.shape[3] // TS
    owned = tile_rows * tile_cols // n
    col_tiles = min(owned, tile_cols)
    width = col_tiles * TS
    per_tile = TS // n
    rows = max(1, owned // tile_cols) * per_tile
    late = LATE if owned == col_tiles and col_tiles > LATE else 0
    pieces = late_pieces(late, per_tile)
    stage, low, high, *edges = exchanged(frames, groups, n, rows, width, width - late * TS, pieces)
    held, heads, tails = (edges[i * len(pieces):(i + 1) * len(pieces)] for i in range(3))
    ups, downs = [(i, i + 1) for i in range(groups - 1)], [(i + 1, i) for i in range(groups - 1)]
    late_edges = [(lax.ppermute(tail, "ta", ups), lax.ppermute(head, "ta", downs)) for head, tail in zip(heads, tails)]
    height = min(per_tile, max(SUBLANES, 256 // n))
    out = smoothed(taps, stage, low, high, groups, (0, owned - late), (0, per_tile), (0, TS), height, col_tiles, owned)
    for (tile, first, count, *cols), cells, (late_low, late_high) in zip(pieces, held, late_edges):
        step = height if count == per_tile else min(SUBLANES, count)
        out = smoothed(
            taps, cells, late_low, late_high, groups, (owned - late + tile, 1), (first, count), cols, step, col_tiles, owned, out)
    return out


def solution(mesh):
    placed = (P("ta", "sa", None, None), P())
    return jax.shard_map(
        on_device, mesh=mesh, in_specs=placed, out_specs=P("sa", "ta", None, None), check_vma=False
    )
```

```python
import functools

import jax
import jax.numpy as jnp
from jax import lax
from jax.experimental import pallas as pl
from jax.experimental.pallas import tpu as pltpu
from jax.sharding import PartitionSpec as P

TS = 512
REACH = 3
SUBLANES = 8
LATE = 2
LATE_UNITS = (2, 1)
LATE_HALVES = 2


def partner(me, m, n, sign):
    if n & (n - 1):
        return (me + sign * m + n) % n
    other, bit = me, 1
    while bit < n:
        if m & bit:
            other = other + bit * (1 - 2 * ((me // bit) % 2))
        bit *= 2
    return other


def greeted_first(order, n):
    if n & (n - 1):
        return order, {}
    near = [m for m in order if m & (m - 1) == 0]
    vouchers = {}
    for m in order:
        if m not in near:
            vouchers.setdefault(next(v for v in order if v & m == v and bin(m ^ v).count("1") == 1), []).append(m)
    return near, vouchers


def late_pieces(late, rows):
    pieces = [(tile, 0, rows, 0, TS) for tile in range(late)]
    units = rows // SUBLANES
    if late and units > sum(LATE_UNITS):
        sizes = (units - sum(LATE_UNITS),) + LATE_UNITS
        pieces[-1:] = [(late - 1, sum(sizes[:i]) * SUBLANES, size * SUBLANES, 0, TS) for i, size in enumerate(sizes)]
        tile, first, count = pieces.pop()[:3]
        pieces += [(tile, first, count, col, TS // LATE_HALVES) for col in range(0, TS, TS // LATE_HALVES)]
    return pieces


def exchange_kernel(groups, n, rows, width, sent, pieces, frames, *refs):
    late = sent < width
    stage, low, high = refs[:3]
    held, heads, tails = (refs[3 + i * len(pieces):3 + (i + 1) * len(pieces)] for i in range(3))
    (own, own_sem, a_send, a_recv, up_send, up_recv, down_send, down_recv,
     next_in, beside_in, near_in) = refs[3 + 3 * len(pieces):][:11]
    if late:
        late_cells, late_load, late_store = refs[-3:]
    steps = frames.shape[0]
    group, me = lax.axis_index("ta"), lax.axis_index("sa")
    across = frames.shape[3] // width
    order = sorted(range(1, n), key=lambda m: (bin(m >> 1).count("1"), m & 1, m))
    parts = [(0, sent), (sent, width - sent)] if late else [(0, width)]
    has_prev, has_next = group > 0, group < groups - 1
    leads = me % 2 == 0
    follows = jnp.logical_not(leads)

    def cells_for(owner, first, count):
        row = pl.ds(pl.multiple_of((owner // across) * rows, 8), rows)
        col = pl.ds(pl.multiple_of((owner % across) * width + first, TS), count)
        return frames.at[:, 0, row, col]

    def await_own():
        @pl.when(has_next)
        def _():
            edge_copy(awaited, "up").wait_send()

        @pl.when(has_prev)
        def _():
            edge_copy(awaited, "down").wait_send()

    opening = min(SUBLANES, rows)
    spans = {0: (0, opening), n: (opening, rows - opening)}
    edges = [m for m in [0, n] + order if spans.get(m, (0, rows))[1]]
    own_edges = [m for m in edges if m in spans]
    awaited = own_edges[-1]
    mine = cells_for(me, *parts[0])
    loads = [
        pltpu.make_async_copy(mine.at[:, pl.ds(*spans[m])], own.at[:, pl.ds(*spans[m])], own_sem.at[1 + i])
        for i, m in enumerate(own_edges)]

    for load in loads:
        load.start()

    near, vouchers = greeted_first(order, n)
    barrier = pltpu.get_barrier_semaphore()

    @pl.when(has_next)
    def _():
        pl.semaphore_signal(barrier, inc=1, device_id={"ta": group + 1})

    @pl.when(jnp.logical_not(has_prev))
    def _():
        for m in near:
            pl.semaphore_signal(barrier, inc=1, device_id={"sa": partner(me, m, n, 1)})


    def block_copy(m, part):
        return pltpu.make_async_remote_copy(
            src_ref=cells_for(partner(me, m, n, 1), *parts[part]), dst_ref=late_cells.at[m] if part else stage.at[me],
            send_sem=a_send.at[part, m], recv_sem=a_recv.at[part, m], device_id={"sa": partner(me, m, n, 1)})

    def edge_copy(m, which):
        source, row = partner(me, m % n, n, -1), pl.ds(*spans.get(m, (0, rows)))
        cells = own if m in spans else stage.at[source]
        if which == "up":
            return pltpu.make_async_remote_copy(
                src_ref=cells.at[pl.ds(steps - REACH, REACH), row], dst_ref=low.at[source, :, row],
                send_sem=up_send.at[m], recv_sem=up_recv.at[m], device_id={"ta": group + 1})
        return pltpu.make_async_remote_copy(
            src_ref=cells.at[pl.ds(0, REACH), row], dst_ref=high.at[source, :, row],
            send_sem=down_send.at[m], recv_sem=down_recv.at[m], device_id={"ta": group - 1})

    def send_edges(m, which=("up", "down")):
        if m not in edges:
            return
        for way in which:
            @pl.when(has_next if way == "up" else has_prev)
            def _():
                edge_copy(m, way).start()

    def late_copies(m):
        source = partner(me, m, n, -1)
        copies = []
        for p, (tile, first, count, left, wide) in enumerate(pieces):
            row, col = pl.ds(first, count), pl.ds(tile * TS + left, wide)
            moves = (
                (pl.ds(0, steps), held[p]), (pl.ds(steps - REACH, REACH), tails[p]), (pl.ds(0, REACH), heads[p]))
            copies += [
                pltpu.make_async_copy(late_cells.at[m, step, row, col], target.at[source], late_store.at[i, p, m])
                for i, (step, target) in enumerate(moves)]
        return copies

    def put_late(m):
        for put in late_copies(m):
            put.start()

    pl.semaphore_wait(barrier, jnp.where(has_prev, 1, len(near)))

    @pl.when(has_prev)
    def _():
        pl.semaphore_signal(next_in, inc=1, device_id={"ta": group - 1})

    for load, m in zip(loads, own_edges):
        load.wait()

        @pl.when(leads)
        def _():
            send_edges(m, ["down"])

    @pl.when(has_next)
    def _():
        pl.semaphore_wait(next_in, 1)

    @pl.when(leads)
    def _():
        send_edges(0, ["up"])
        send_edges(n, ["up"])

    @pl.when(has_prev)
    def _():
        pl.semaphore_wait(near_in, 1)

    for m in near[1:]:
        block_copy(m, 0).start()

    @pl.when(follows)
    def _():
        block_copy(order[0], 0).start()

    @pl.when(has_next)
    def _():
        for m in near:
            pl.semaphore_signal(beside_in, inc=1, device_id={"sa": partner(me, m, n, 1)})
        pl.semaphore_wait(beside_in, len(near))
        pl.semaphore_signal(near_in, inc=1, device_id={"ta": group + 1})

    store = pltpu.make_async_copy(own, stage.at[me], own_sem.at[0])
    store.start()
    if late:
        late_own = pltpu.make_async_copy(cells_for(me, *parts[1]), late_cells.at[0], late_load.at[0])
        late_own.start()
    for m in order:
        block_copy(m, 0).wait_recv()
        if m == order[0]:
            @pl.when(follows)
            def _():
                send_edges(0)
                send_edges(n)
        send_edges(m)
        if m == order[0]:
            @pl.when(leads)
            def _():
                await_own()
                block_copy(m, 0).start()

        for other in vouchers.get(m, []):
            block_copy(other, 0).start()
    if late:
        for m in order:
            block_copy(m, 1).start()
        late_own.wait()
        put_late(0)
        for m in order:
            block_copy(m, 1).wait_recv()
            put_late(m)
    store.wait()
    if late:
        for m in [0] + order:
            for put in late_copies(m):
                put.wait()
    for part in range(len(parts)):
        for m in order:
            block_copy(m, part).wait_send()
    @pl.when(follows)
    def _():
        await_own()

    for m in edges:
        @pl.when(has_next)
        def _():
            if m != awaited:
                edge_copy(m, "up").wait_send()
            edge_copy(m, "down").wait_recv()

        @pl.when(has_prev)
        def _():
            if m != awaited:
                edge_copy(m, "down").wait_send()
            edge_copy(m, "up").wait_recv()


def exchanged(frames, groups, n, rows, width, sent, pieces):
    steps = frames.shape[0]
    any_space = pl.BlockSpec(memory_space=pl.ANY)
    edge = jax.ShapeDtypeStruct((n, REACH, rows, sent), jnp.float32)
    dma, block_dma = pltpu.SemaphoreType.DMA((n + 1,)), pltpu.SemaphoreType.DMA((2, n))
    shapes = [jax.ShapeDtypeStruct((n, steps, rows, sent), jnp.float32), edge, edge]
    scratch = [pltpu.VMEM((steps, rows, sent), jnp.float32), pltpu.SemaphoreType.DMA((3,)), block_dma, block_dma] + [dma] * 4
    scratch += [pltpu.SemaphoreType.REGULAR] * 3
    if pieces:
        shapes += [
            jax.ShapeDtypeStruct((n, depth, count, wide), jnp.float32)
            for depth in (steps, REACH, REACH) for _, _, count, _, wide in pieces]
        scratch += [
            pltpu.VMEM((n, steps, rows, width - sent), jnp.float32), pltpu.SemaphoreType.DMA((1,)),
            pltpu.SemaphoreType.DMA((3, len(pieces), n))]
    return pl.pallas_call(
        functools.partial(exchange_kernel, groups, n, rows, width, sent, pieces),
        out_shape=shapes,
        in_specs=[any_space],
        out_specs=[any_space] * len(shapes),
        scratch_shapes=scratch,
        compiler_params=pltpu.CompilerParams(collective_id=0, has_side_effects=True),
        name="exchange",
    )(frames)


def smooth_kernel(groups, taps, stage, low, high, *rest):
    out, woven = rest[-2:]
    n, steps, rows, cols = stage.shape
    group = lax.axis_index("ta")
    first, last = group == 0, group == groups - 1
    weights = [jnp.broadcast_to(taps[:, j:j + 1], (8, 128)) for j in range(2 * REACH + 1)]

    for c in range(0, cols, 128):
        lanes = pl.ds(c, 128)

        def one_source(s, carry):
            for r in range(0, rows, 8):
                at = (pl.ds(r, 8), lanes)
                lo = [jnp.where(first, 0.0, low[(s, j) + at]) for j in range(REACH)]
                hi = [jnp.where(last, 0.0, high[(s, j) + at]) for j in range(REACH)]
                cells = lo + [stage[(s, t) + at] for t in range(steps)] + hi
                for t in range(steps):
                    total = weights[0] * cells[t]
                    for j in range(1, 2 * REACH + 1):
                        total = total + weights[j] * cells[t + j]
                    woven[t, pl.ds(r * n + s, 8, stride=n), :] = total
            return carry

        if rows == SUBLANES and n <= SUBLANES:
            for s in range(n):
                one_source(s, 0)
        else:
            lax.fori_loop(0, n, one_source, 0)
        for t in range(steps):
            out[t, :, lanes] = woven[t]


def smoothed(taps, stage, low, high, groups, tiles, band, cols, height, col_tiles, owned, into=None):
    n, steps = stage.shape[:2]
    (start, count), (first, span), (left, wide) = tiles, band, cols
    splits, above = (TS // n) // height, first // height

    def cells_at(k, h):
        if into is not None:
            return 0, 0, h, 0
        return 0, 0, ((k + start) // col_tiles) * splits + h, (k + start) % col_tiles

    specs = [
        pl.BlockSpec(memory_space=pltpu.VMEM),
        pl.BlockSpec((n, steps, height, wide), cells_at),
        pl.BlockSpec((n, REACH, height, wide), cells_at),
        pl.BlockSpec((n, REACH, height, wide), cells_at),
    ]
    operands = [taps.reshape(1, -1), stage, low, high]
    if into is not None:
        specs.append(pl.BlockSpec(memory_space=pl.ANY))
        operands.append(into)
    moved = count * steps * span * n * wide * 4
    return pl.pallas_call(
        functools.partial(smooth_kernel, groups),
        grid=(count, span // height),
        out_shape=jax.ShapeDtypeStruct((owned, steps, TS, TS), jnp.float32),
        in_specs=specs,
        out_specs=pl.BlockSpec((None, steps, height * n, wide), lambda k, h: (k + start, 0, above + h, left // wide)),
        scratch_shapes=[pltpu.VMEM((steps, height * n, 128), jnp.float32)],
        input_output_aliases={} if into is None else {4: 0},
        compiler_params=pltpu.CompilerParams(vmem_limit_bytes=(40 if height > SUBLANES else 8) * 1024 * 1024),
        cost_estimate=pl.CostEstimate(flops=moved * 4, bytes_accessed=moved * 7 // 2, transcendentals=0),
        name="smooth",
    )(*operands)


def on_device(frames, taps):
    groups, n = lax.axis_size("ta"), lax.axis_size("sa")
    tile_rows, tile_cols = frames.shape[2] * n // TS, frames.shape[3] // TS
    owned = tile_rows * tile_cols // n
    col_tiles = min(owned, tile_cols)
    width = col_tiles * TS
    per_tile = TS // n
    rows = max(1, owned // tile_cols) * per_tile
    late = LATE if owned == col_tiles and col_tiles > LATE else 0
    pieces = late_pieces(late, per_tile)
    stage, low, high, *edges = exchanged(frames, groups, n, rows, width, width - late * TS, pieces)
    held, heads, tails = (edges[i * len(pieces):(i + 1) * len(pieces)] for i in range(3))
    ups, downs = [(i, i + 1) for i in range(groups - 1)], [(i + 1, i) for i in range(groups - 1)]
    late_edges = [(lax.ppermute(tail, "ta", ups), lax.ppermute(head, "ta", downs)) for head, tail in zip(heads, tails)]
    height = min(per_tile, max(SUBLANES, 256 // n))
    out = smoothed(taps, stage, low, high, groups, (0, owned - late), (0, per_tile), (0, TS), height, col_tiles, owned)
    for (tile, first, count, *cols), cells, (late_low, late_high) in zip(pieces, held, late_edges):
        step = height if count == per_tile else min(SUBLANES, count)
        out = smoothed(
            taps, cells, late_low, late_high, groups, (owned - late + tile, 1), (first, count), cols, step, col_tiles, owned, out)
    return out


def solution(mesh):
    placed = (P("ta", "sa", None, None), P())
    return jax.shard_map(
        on_device, mesh=mesh, in_specs=placed, out_specs=P("sa", "ta", None, None), check_vma=False
    )
```

```python
import functools

import jax
import jax.numpy as jnp
from jax import lax
from jax.experimental import pallas as pl
from jax.experimental.pallas import tpu as pltpu
from jax.sharding import PartitionSpec as P

TS = 512
REACH = 3
SUBLANES = 8
LATE = 2
LATE_UNITS = (2, 1)
LATE_CUTS = 4


def partner(me, m, n, sign):
    if n & (n - 1):
        return (me + sign * m + n) % n
    other, bit = me, 1
    while bit < n:
        if m & bit:
            other = other + bit * (1 - 2 * ((me // bit) % 2))
        bit *= 2
    return other


def greeted_first(order, n):
    if n & (n - 1):
        return order, {}
    near = [m for m in order if m & (m - 1) == 0]
    vouchers = {}
    for m in order:
        if m not in near:
            vouchers.setdefault(next(v for v in order if v & m == v and bin(m ^ v).count("1") == 1), []).append(m)
    return near, vouchers


def late_pieces(late, rows):
    pieces = [(tile, 0, rows, 0, TS) for tile in range(late)]
    units = rows // SUBLANES
    if late and units > sum(LATE_UNITS):
        sizes = (units - sum(LATE_UNITS),) + LATE_UNITS
        pieces[-1:] = [(late - 1, sum(sizes[:i]) * SUBLANES, size * SUBLANES, 0, TS) for i, size in enumerate(sizes)]
        tile, first, count = pieces.pop()[:3]
        pieces += [(tile, first, count, col, TS // LATE_CUTS) for col in range(0, TS, TS // LATE_CUTS)]
    return pieces


def exchange_kernel(groups, n, rows, width, sent, pieces, frames, *refs):
    late = sent < width
    stage, low, high = refs[:3]
    held, heads, tails = (refs[3 + i * len(pieces):3 + (i + 1) * len(pieces)] for i in range(3))
    (own, own_sem, a_send, a_recv, up_send, up_recv, down_send, down_recv,
     next_in, beside_in, near_in) = refs[3 + 3 * len(pieces):][:11]
    if late:
        late_cells, late_load, late_store = refs[-3:]
    steps = frames.shape[0]
    group, me = lax.axis_index("ta"), lax.axis_index("sa")
    across = frames.shape[3] // width
    order = sorted(range(1, n), key=lambda m: (bin(m >> 1).count("1"), m & 1, m))
    parts = [(0, sent), (sent, width - sent)] if late else [(0, width)]
    has_prev, has_next = group > 0, group < groups - 1
    leads = me % 2 == 0
    follows = jnp.logical_not(leads)

    def cells_for(owner, first, count):
        row = pl.ds(pl.multiple_of((owner // across) * rows, 8), rows)
        col = pl.ds(pl.multiple_of((owner % across) * width + first, TS), count)
        return frames.at[:, 0, row, col]

    def await_own():
        @pl.when(has_next)
        def _():
            edge_copy(awaited, "up").wait_send()

        @pl.when(has_prev)
        def _():
            edge_copy(awaited, "down").wait_send()

    opening = min(SUBLANES, rows)
    spans = {0: (0, opening), n: (opening, rows - opening)}
    edges = [m for m in [0, n] + order if spans.get(m, (0, rows))[1]]
    own_edges = [m for m in edges if m in spans]
    awaited = own_edges[-1]
    mine = cells_for(me, *parts[0])
    loads = [
        pltpu.make_async_copy(mine.at[:, pl.ds(*spans[m])], own.at[:, pl.ds(*spans[m])], own_sem.at[1 + i])
        for i, m in enumerate(own_edges)]

    for load in loads:
        load.start()

    near, vouchers = greeted_first(order, n)
    barrier = pltpu.get_barrier_semaphore()

    @pl.when(has_next)
    def _():
        pl.semaphore_signal(barrier, inc=1, device_id={"ta": group + 1})

    @pl.when(jnp.logical_not(has_prev))
    def _():
        for m in near:
            pl.semaphore_signal(barrier, inc=1, device_id={"sa": partner(me, m, n, 1)})


    def block_copy(m, part):
        return pltpu.make_async_remote_copy(
            src_ref=cells_for(partner(me, m, n, 1), *parts[part]), dst_ref=late_cells.at[m] if part else stage.at[me],
            send_sem=a_send.at[part, m], recv_sem=a_recv.at[part, m], device_id={"sa": partner(me, m, n, 1)})

    def edge_copy(m, which):
        source, row = partner(me, m % n, n, -1), pl.ds(*spans.get(m, (0, rows)))
        cells = own if m in spans else stage.at[source]
        if which == "up":
            return pltpu.make_async_remote_copy(
                src_ref=cells.at[pl.ds(steps - REACH, REACH), row], dst_ref=low.at[source, :, row],
                send_sem=up_send.at[m], recv_sem=up_recv.at[m], device_id={"ta": group + 1})
        return pltpu.make_async_remote_copy(
            src_ref=cells.at[pl.ds(0, REACH), row], dst_ref=high.at[source, :, row],
            send_sem=down_send.at[m], recv_sem=down_recv.at[m], device_id={"ta": group - 1})

    def send_edges(m, which=("up", "down")):
        if m not in edges:
            return
        for way in which:
            @pl.when(has_next if way == "up" else has_prev)
            def _():
                edge_copy(m, way).start()

    def late_copies(m):
        source = partner(me, m, n, -1)
        copies = []
        for p, (tile, first, count, left, wide) in enumerate(pieces):
            row, col = pl.ds(first, count), pl.ds(tile * TS + left, wide)
            moves = (
                (pl.ds(0, steps), held[p]), (pl.ds(steps - REACH, REACH), tails[p]), (pl.ds(0, REACH), heads[p]))
            copies += [
                pltpu.make_async_copy(late_cells.at[m, step, row, col], target.at[source], late_store.at[i, p, m])
                for i, (step, target) in enumerate(moves)]
        return copies

    def put_late(m):
        for put in late_copies(m):
            put.start()

    pl.semaphore_wait(barrier, jnp.where(has_prev, 1, len(near)))

    @pl.when(has_prev)
    def _():
        pl.semaphore_signal(next_in, inc=1, device_id={"ta": group - 1})

    for load, m in zip(loads, own_edges):
        load.wait()

        @pl.when(leads)
        def _():
            send_edges(m, ["down"])

        if m == own_edges[0]:
            @pl.when(has_next)
            def _():
                pl.semaphore_wait(next_in, 1)

        @pl.when(leads)
        def _():
            send_edges(m, ["up"])

    @pl.when(has_prev)
    def _():
        pl.semaphore_wait(near_in, 1)

    for m in near[1:]:
        block_copy(m, 0).start()

    @pl.when(follows)
    def _():
        block_copy(order[0], 0).start()

    @pl.when(has_next)
    def _():
        for m in near:
            pl.semaphore_signal(beside_in, inc=1, device_id={"sa": partner(me, m, n, 1)})
        pl.semaphore_wait(beside_in, len(near))
        pl.semaphore_signal(near_in, inc=1, device_id={"ta": group + 1})

    store = pltpu.make_async_copy(own, stage.at[me], own_sem.at[0])
    store.start()
    if late:
        late_own = pltpu.make_async_copy(cells_for(me, *parts[1]), late_cells.at[0], late_load.at[0])
        late_own.start()
    for m in order:
        block_copy(m, 0).wait_recv()
        if m == order[0]:
            @pl.when(follows)
            def _():
                send_edges(0)
                send_edges(n)
        send_edges(m)
        if m == order[0]:
            @pl.when(leads)
            def _():
                await_own()
                block_copy(m, 0).start()

        for other in vouchers.get(m, []):
            block_copy(other, 0).start()
    if late:
        for m in order:
            block_copy(m, 1).start()
        late_own.wait()
        put_late(0)
        for m in order:
            block_copy(m, 1).wait_recv()
            put_late(m)
    store.wait()
    if late:
        for m in [0] + order:
            for put in late_copies(m):
                put.wait()
    for part in range(len(parts)):
        for m in order:
            block_copy(m, part).wait_send()
    @pl.when(follows)
    def _():
        await_own()

    for m in edges:
        @pl.when(has_next)
        def _():
            if m != awaited:
                edge_copy(m, "up").wait_send()
            edge_copy(m, "down").wait_recv()

        @pl.when(has_prev)
        def _():
            if m != awaited:
                edge_copy(m, "down").wait_send()
            edge_copy(m, "up").wait_recv()


def exchanged(frames, groups, n, rows, width, sent, pieces):
    steps = frames.shape[0]
    any_space = pl.BlockSpec(memory_space=pl.ANY)
    edge = jax.ShapeDtypeStruct((n, REACH, rows, sent), jnp.float32)
    dma, block_dma = pltpu.SemaphoreType.DMA((n + 1,)), pltpu.SemaphoreType.DMA((2, n))
    shapes = [jax.ShapeDtypeStruct((n, steps, rows, sent), jnp.float32), edge, edge]
    scratch = [pltpu.VMEM((steps, rows, sent), jnp.float32), pltpu.SemaphoreType.DMA((3,)), block_dma, block_dma] + [dma] * 4
    scratch += [pltpu.SemaphoreType.REGULAR] * 3
    if pieces:
        shapes += [
            jax.ShapeDtypeStruct((n, depth, count, wide), jnp.float32)
            for depth in (steps, REACH, REACH) for _, _, count, _, wide in pieces]
        scratch += [
            pltpu.VMEM((n, steps, rows, width - sent), jnp.float32), pltpu.SemaphoreType.DMA((1,)),
            pltpu.SemaphoreType.DMA((3, len(pieces), n))]
    return pl.pallas_call(
        functools.partial(exchange_kernel, groups, n, rows, width, sent, pieces),
        out_shape=shapes,
        in_specs=[any_space],
        out_specs=[any_space] * len(shapes),
        scratch_shapes=scratch,
        compiler_params=pltpu.CompilerParams(collective_id=0, has_side_effects=True),
        name="exchange",
    )(frames)


def smooth_kernel(groups, taps, stage, low, high, *rest):
    out, woven = rest[-2:]
    n, steps, rows, cols = stage.shape
    group = lax.axis_index("ta")
    first, last = group == 0, group == groups - 1
    weights = [jnp.broadcast_to(taps[:, j:j + 1], (8, 128)) for j in range(2 * REACH + 1)]

    for c in range(0, cols, 128):
        lanes = pl.ds(c, 128)

        def one_source(s, carry):
            for r in range(0, rows, 8):
                at = (pl.ds(r, 8), lanes)
                lo = [jnp.where(first, 0.0, low[(s, j) + at]) for j in range(REACH)]
                hi = [jnp.where(last, 0.0, high[(s, j) + at]) for j in range(REACH)]
                cells = lo + [stage[(s, t) + at] for t in range(steps)] + hi
                for t in range(steps):
                    total = weights[0] * cells[t]
                    for j in range(1, 2 * REACH + 1):
                        total = total + weights[j] * cells[t + j]
                    woven[t, pl.ds(r * n + s, 8, stride=n), :] = total
            return carry

        if rows == SUBLANES and n <= SUBLANES:
            for s in range(n):
                one_source(s, 0)
        else:
            lax.fori_loop(0, n, one_source, 0)
        for t in range(steps):
            out[t, :, lanes] = woven[t]


def smoothed(taps, stage, low, high, groups, tiles, band, cols, height, col_tiles, owned, into=None):
    n, steps = stage.shape[:2]
    (start, count), (first, span), (left, wide) = tiles, band, cols
    splits, above = (TS // n) // height, first // height

    def cells_at(k, h):
        if into is not None:
            return 0, 0, h, 0
        return 0, 0, ((k + start) // col_tiles) * splits + h, (k + start) % col_tiles

    specs = [
        pl.BlockSpec(memory_space=pltpu.VMEM),
        pl.BlockSpec((n, steps, height, wide), cells_at),
        pl.BlockSpec((n, REACH, height, wide), cells_at),
        pl.BlockSpec((n, REACH, height, wide), cells_at),
    ]
    operands = [taps.reshape(1, -1), stage, low, high]
    if into is not None:
        specs.append(pl.BlockSpec(memory_space=pl.ANY))
        operands.append(into)
    moved = count * steps * span * n * wide * 4
    return pl.pallas_call(
        functools.partial(smooth_kernel, groups),
        grid=(count, span // height),
        out_shape=jax.ShapeDtypeStruct((owned, steps, TS, TS), jnp.float32),
        in_specs=specs,
        out_specs=pl.BlockSpec((None, steps, height * n, wide), lambda k, h: (k + start, 0, above + h, left // wide)),
        scratch_shapes=[pltpu.VMEM((steps, height * n, 128), jnp.float32)],
        input_output_aliases={} if into is None else {4: 0},
        compiler_params=pltpu.CompilerParams(vmem_limit_bytes=(40 if height > SUBLANES else 8) * 1024 * 1024),
        cost_estimate=pl.CostEstimate(flops=moved * 4, bytes_accessed=moved * 7 // 2, transcendentals=0),
        name="smooth",
    )(*operands)


def on_device(frames, taps):
    groups, n = lax.axis_size("ta"), lax.axis_size("sa")
    tile_rows, tile_cols = frames.shape[2] * n // TS, frames.shape[3] // TS
    owned = tile_rows * tile_cols // n
    col_tiles = min(owned, tile_cols)
    width = col_tiles * TS
    per_tile = TS // n
    rows = max(1, owned // tile_cols) * per_tile
    late = LATE if owned == col_tiles and col_tiles > LATE else 0
    pieces = late_pieces(late, per_tile)
    stage, low, high, *edges = exchanged(frames, groups, n, rows, width, width - late * TS, pieces)
    held, heads, tails = (edges[i * len(pieces):(i + 1) * len(pieces)] for i in range(3))
    ups, downs = [(i, i + 1) for i in range(groups - 1)], [(i + 1, i) for i in range(groups - 1)]
    late_edges = [(lax.ppermute(tail, "ta", ups), lax.ppermute(head, "ta", downs)) for head, tail in zip(heads, tails)]
    height = min(per_tile, max(SUBLANES, 256 // n))
    out = smoothed(taps, stage, low, high, groups, (0, owned - late), (0, per_tile), (0, TS), height, col_tiles, owned)
    for (tile, first, count, *cols), cells, (late_low, late_high) in zip(pieces, held, late_edges):
        step = height if count == per_tile else min(SUBLANES, count)
        out = smoothed(
            taps, cells, late_low, late_high, groups, (owned - late + tile, 1), (first, count), cols, step, col_tiles, owned, out)
    return out


def solution(mesh):
    placed = (P("ta", "sa", None, None), P())
    return jax.shard_map(
        on_device, mesh=mesh, in_specs=placed, out_specs=P("sa", "ta", None, None), check_vma=False
    )
```
